32 devices in a mesh: rows: 32 (over z, y, x, core).
Axes of the slice: x: 2, y: 2, z: 4, core: 2. Of those that a mesh axis runs over, the one named last changes fastest.
Arguments:
- snapshots: float32 [16384, 512], P('rows'), may hold values from -100 to 100
- validation: float32 [16384, 512], P('rows'), may hold values from -100 to 100
- eigenvectors: float32 [512, 64], replicated, may hold values from -0.25 to 0.25
- eigenvalues: float32 [64], replicated, may hold values from 16 to 256
Outputs:
- gram: float32 [512, 512], replicated
- modes: float32 [64, 16384], P(None, 'rows')
- train_coef: float32 [64, 512], replicated
- valid_coef: float32 [64, 512], replicated
The draws below stay inside these ranges and needn't reach their ends.
All inputs are finite; a program needn't handle non-finite values.
Results may differ from the reference program's by a relative error of at most 0.000071.
Values sent between devices are 32-bit elements; how exact they have to be, the bound alone decides.
No kernel may reach another device: no remote copies, remote signals or barrier semaphores. Data moves between devices by JAX's collectives and lax.ppermute only.
A program may use at most 64 MiB of HBM per device.

```python
import math
import jax
import jax.numpy as jnp
from jax import lax

K = 512
M = 64
NDOF = 16384


def common_parts(key):
    base = jax.random.fold_in(key, 7)
    first, second, third = jax.random.split(base, 3)
    spread = jnp.exp(jax.random.uniform(first, (NDOF, 1), jnp.float32, 0.0, 0.5 * math.log(10.0)))
    rising = jnp.sqrt(1.0 + 2.0 * jnp.arange(NDOF, dtype=jnp.float32) / NDOF)[:, None]
    columns = jnp.exp(jax.random.uniform(third, (1, K), jnp.float32, 0.0, 0.25 * math.log(10.0)))
    noise = jnp.clip(jax.random.normal(second, (NDOF, K), jnp.float32), -6.0, 6.0)
    return (spread * rising * columns, noise)


def draw_snapshots(key, part):
    scaling, noise = common_parts(key)
    return scaling * noise


def draw_validation(key, part):
    scaling, noise = common_parts(key)
    other = jax.random.fold_in(key, 11)
    fresh = jnp.clip(jax.random.normal(other, (NDOF, K), jnp.float32), -6.0, 6.0)
    return scaling * (0.8 * noise + 0.6 * fresh)


def centred(rng, extent, scale, limit, kind=jnp.bfloat16):
    entries = scale * jax.random.normal(rng, extent, jnp.float32)
    return jnp.clip(entries, min=-limit, max=limit).astype(kind)


def setup_inputs(seed: int = 0) -> dict:
    arg_keys = jax.random.split(jax.random.key(seed), 5)
    snapshots = draw_snapshots(jax.random.fold_in(arg_keys[4], 71), 0)
    validation = draw_validation(jax.random.fold_in(arg_keys[4], 71), 0)
    eigenvectors = centred(arg_keys[2], (K, M), K ** -0.5, 0.25, jnp.float32)
    eigenvalues = jnp.clip(jnp.exp(jax.random.uniform(arg_keys[3], (M,), jnp.float32, math.log(16.0), math.log(256.0))), 16.0, 256.0)
    return {"snapshots": snapshots, "validation": validation, "eigenvectors": eigenvectors, "eigenvalues": eigenvalues}


def reference(snapshots, validation, eigenvectors, eigenvalues):
    highest = lax.Precision.HIGHEST
    total = snapshots.shape[0] * 1.0
    gram = lax.dot_general(snapshots, snapshots, (((0,), (0,)), ((), ())), precision=highest, preferred_element_type=jnp.float32) / total
    scales = lax.rsqrt(eigenvalues)
    modes = lax.dot_general(eigenvectors, snapshots, (((0,), (1,)), ((), ())), precision=highest, preferred_element_type=jnp.float32) * scales[:, None]
    train_coef = jnp.dot(modes, snapshots, precision=highest, preferred_element_type=jnp.float32) / total
    valid_coef = jnp.dot(modes, validation, precision=highest, preferred_element_type=jnp.float32) / total
    return (gram, modes, train_coef, valid_coef)
```

```python
import jax
import jax.numpy as jnp
from jax import lax
from jax.sharding import Mesh, PartitionSpec as P

BLOCK = 128
DIRECT = 4


def axes_of(mesh):
    devices = list(mesh.devices.flat)
    cores = len({d.core_on_chip for d in devices})
    planes = len({d.coords[2] for d in devices})
    chips = len(devices) // (cores * planes)
    return Mesh(mesh.devices.reshape(planes, chips, cores), ("plane", "chip", "core"))


def partners(n, r):
    return [(i, i ^ r) for i in range(n)]


def tree(parts):
    while len(parts) > 1:
        parts = [a + b for a, b in zip(parts[::2], parts[1::2], strict=True)]
    return parts[0]


def direct(n):
    return n <= DIRECT and n & (n - 1) == 0


def reduce_scatter(x, axis):
    n = lax.axis_size(axis)
    if not direct(n):
        return lax.psum_scatter(x, axis)
    me = lax.axis_index(axis)
    parts = [lax.dynamic_index_in_dim(x, me ^ r, 0, False) for r in range(n)]
    return tree([p if r == 0 else lax.ppermute(p, axis, partners(n, r)) for r, p in enumerate(parts)])


def all_reduce(x, axis):
    n = lax.axis_size(axis)
    if not direct(n):
        return lax.psum(x, axis)
    return tree([x if r == 0 else lax.ppermute(x, axis, partners(n, r)) for r in range(n)])


def body(snapshots, validation, eigenvectors, eigenvalues):
    high = lax.Precision.HIGH
    cores, chips = lax.axis_size("core"), lax.axis_size("chip")
    devices = cores * chips * lax.axis_size("plane")
    total = snapshots.shape[0] * devices * 1.0
    k, m = eigenvectors.shape
    blocks = k // BLOCK
    dot = lambda a, b, dims, p: lax.dot_general(a, b, (dims, ((), ())), precision=p, preferred_element_type=jnp.float32)
    scales = lax.rsqrt(eigenvalues)
    gram_part = dot(snapshots, snapshots, ((0,), (0,)), high) / total
    modes = dot(eigenvectors, snapshots, ((0,), (1,)), high) * scales[:, None]
    valid_part = dot(modes, validation, ((1,), (0,)), high) / total

    upper = [(i, j) for i in range(blocks) for j in range(i, blocks)]
    cut = lambda a, i, j: a[i * BLOCK : (i + 1) * BLOCK, j * BLOCK : (j + 1) * BLOCK]
    packed = jnp.concatenate([cut(gram_part, i, j) for i, j in upper] + [valid_part[:, j * BLOCK : (j + 1) * BLOCK] for j in range(blocks)], 0)
    rows = packed.shape[0]
    piece = -(-rows // (cores * chips * 8)) * 8
    packed = jnp.pad(packed, ((0, cores * chips * piece - rows), (0, 0)))

    own = reduce_scatter(packed.reshape(chips, cores, piece, BLOCK).swapaxes(0, 1), "core")
    own = reduce_scatter(own, "chip")
    own = all_reduce(own, "plane")
    packed = lax.all_gather(own, ("chip", "core"), tiled=True)

    at = {ij: packed[n * BLOCK : (n + 1) * BLOCK] for n, ij in enumerate(upper)}
    gram = jnp.concatenate(
        [jnp.concatenate([at[i, j] if i <= j else at[j, i].T for j in range(blocks)], 1) for i in range(blocks)], 0
    )
    base = len(upper) * BLOCK
    valid_coef = jnp.concatenate([packed[base + j * m : base + (j + 1) * m] for j in range(blocks)], 1)
    train_coef = dot(eigenvectors, gram, ((0,), (0,)), high) * scales[:, None]
    return gram, modes, train_coef, valid_coef


def solution(mesh):
    inner = axes_of(mesh)
    rows = ("plane", "chip", "core")
    in_specs = (P(rows, None), P(rows, None), P(), P())
    out_specs = (P(), P(None, rows), P(), P())
    return jax.shard_map(body, mesh=inner, in_specs=in_specs, out_specs=out_specs, check_vma=False)
```

```python
import functools

import jax
import jax.numpy as jnp
from jax import lax
from jax.experimental import pallas as pl
from jax.experimental.pallas import tpu as pltpu
from jax.sharding import Mesh, PartitionSpec as P

LANES = 128
DIRECT = 4
F32 = jnp.float32


def axes_of(mesh):
    devices = list(mesh.devices.flat)
    cores = len({d.core_on_chip for d in devices})
    planes = len({d.coords[2] for d in devices})
    chips = len(devices) // (cores * planes)
    return Mesh(mesh.devices.reshape(planes, chips, cores), ("plane", "chip", "core"))


def layout(k, m):
    half = k // 2
    square = half * half // LANES
    mixed, cross, valid = 0, square, 2 * square
    diagonal = valid + m * k // LANES
    return mixed, cross, valid, diagonal, diagonal + half // LANES


def split(x):
    high = x.astype(jnp.bfloat16)
    return high, (x - high.astype(F32)).astype(jnp.bfloat16)


def dot(a, b, ca, cb):
    return lax.dot_general(a, b, (((ca,), (cb,)), ((), ())), preferred_element_type=F32)


def column(row, m):
    r, c = (lax.broadcasted_iota(jnp.int32, (m, m), d) for d in (0, 1))
    return jnp.sum(jnp.where(r == c, jnp.broadcast_to(row, (m, m)), 0.0), axis=1, keepdims=True)


def order(half):
    r, c = (lax.broadcasted_iota(jnp.int32, (half, half), d) for d in (0, 1))
    return r, c


def head_kernel(
    total, s_hbm, v_hbm, e_hbm, w_hbm, packed_ref, modes_hbm, e_out, scale_out, s_buf, v_buf, e_buf, w_buf, modes_ref, sems
):
    n, k = s_buf.shape
    m = e_buf.shape[0]
    half, step = k // 2, n // 2
    mixed, cross, valid, diagonal, rows = layout(k, m)
    copies = []
    halves = [pl.ds(i * step, step) for i in range(2)]
    for src, buf in [
        *((s_hbm.at[at], s_buf.at[at]) for at in halves), (e_hbm, e_buf), (w_hbm, w_buf),
        *((v_hbm.at[at], v_buf.at[at]) for at in halves),
    ]:
        copies.append(pltpu.make_async_copy(src, buf, sems.at[len(copies)]))
        copies[-1].start()
    a = b = c = None
    modes = []
    for i in range(2):
        copies[i].wait()
        high, low = split(s_buf[i * step : (i + 1) * step, :])
        ha, hb, la, lb = high[:, :half], high[:, half:], low[:, :half], low[:, half:]
        da = dot(ha, ha, 0, 0) + dot(ha, la, 0, 0) + dot(la, ha, 0, 0)
        db = dot(ha, hb, 0, 0) + dot(ha, lb, 0, 0) + dot(la, hb, 0, 0)
        dc = dot(hb, hb, 0, 0) + dot(hb, lb, 0, 0) + dot(lb, hb, 0, 0)
        a, b, c = (da, db, dc) if i == 0 else (a + da, b + db, c + dc)
        if i == 0:
            copies[2].wait()
            copies[3].wait()
            scales = column(lax.rsqrt(w_buf[...]), m)
            e_high, e_low = split(e_buf[...])
            e_both = jnp.concatenate([e_high, e_low], 0)
            e_out[...] = e_both
            scale_out[...] = jnp.broadcast_to(scales, scale_out.shape)
        both = dot(e_both, high, 1, 1)
        modes.append((both[:m] + both[m:] + dot(e_high, low, 1, 1)) * scales)
        modes_ref[:, i * step : (i + 1) * step] = modes[i]
    modes_out = pltpu.make_async_copy(modes_ref, modes_hbm, sems.at[6])
    modes_out.start()
    r, col = order(half)
    square = jnp.where(col >= r, a, c) * (1.0 / total)
    b = b * (1.0 / total)
    last = jnp.sum(jnp.where(col == r, c, 0.0), axis=0, keepdims=True) * (1.0 / total)
    for j in range(half // LANES):
        lanes = slice(j * LANES, (j + 1) * LANES)
        packed_ref[mixed + j * half : mixed + (j + 1) * half, :] = square[:, lanes]
        packed_ref[cross + j * half : cross + (j + 1) * half, :] = b[:, lanes]
    pad = packed_ref.shape[0] - diagonal
    packed_ref[diagonal:, :] = jnp.concatenate(
        [last[:, j * LANES : (j + 1) * LANES] for j in range(half // LANES)]
        + [jnp.zeros((pad - half // LANES, LANES), F32)], 0
    )
    out = None
    for i in range(2):
        copies[4 + i].wait()
        m_high, m_low = split(modes[i])
        v_high, v_low = split(v_buf[i * step : (i + 1) * step, :])
        both = dot(jnp.concatenate([m_high, m_low], 0), v_high, 1, 0)
        part = both[:m] + both[m:] + dot(m_high, v_low, 1, 0)
        out = part if i == 0 else out + part
    out = out * (1.0 / total)
    for j in range(k // LANES):
        packed_ref[valid + j * m : valid + (j + 1) * m, :] = out[:, j * LANES : (j + 1) * LANES]
    modes_out.wait()


def in_hbm(x):
    return pltpu.with_memory_space_constraint(x, pltpu.HBM)


def head(snapshots, validation, e_rows, w_row, total, rows):
    n, k = snapshots.shape
    m = e_rows.shape[0]
    hbm, vmem = pl.BlockSpec(memory_space=pltpu.HBM), pl.BlockSpec(memory_space=pltpu.VMEM)
    return pl.pallas_call(
        functools.partial(head_kernel, total),
        out_shape=(
            pltpu.VMEM((rows, LANES), F32), pltpu.HBM((m, n), F32),
            pltpu.VMEM((2 * m, k), jnp.bfloat16), pltpu.VMEM((m, LANES), F32),
        ),
        in_specs=[hbm] * 4,
        out_specs=(vmem, hbm, vmem, vmem),
        scratch_shapes=[
            pltpu.VMEM((n, k), F32), pltpu.VMEM((n, k), F32), pltpu.VMEM((m, k), F32), pltpu.VMEM((1, m), F32),
            pltpu.VMEM((m, n), F32), pltpu.SemaphoreType.DMA((7,)),
        ],
        compiler_params=pltpu.CompilerParams(vmem_limit_bytes=24 * 1024 * 1024),
        name="head",
    )(in_hbm(snapshots), in_hbm(validation), in_hbm(e_rows), in_hbm(w_row))


def tail_kernel(packed_ref, e_ref, scale_ref, gram_hbm, train_hbm, valid_hbm, gram, train_ref, sems):
    m, k = train_ref.shape
    half = k // 2
    mixed, cross, valid, diagonal, _ = layout(k, m)
    tiles = half // LANES
    sent = []

    def send(src, dst):
        sent.append(pltpu.make_async_copy(src, dst, sems.at[len(sent)]))
        sent[-1].start()

    for j in range(k // LANES):
        send(packed_ref.at[pl.ds(valid + j * m, m)], valid_hbm.at[:, pl.ds(j * LANES, LANES)])
    get = lambda first, j: packed_ref[first + j * half : first + (j + 1) * half, :]
    square = jnp.concatenate([get(mixed, j) for j in range(tiles)], 1)
    b = jnp.concatenate([get(cross, j) for j in range(tiles)], 1)
    last = jnp.concatenate([packed_ref[diagonal + j : diagonal + j + 1, :] for j in range(tiles)], 1)
    r, col = order(half)
    turned = square.T
    gram[:half, :half] = jnp.where(col >= r, square, turned)
    gram[:half, half:] = b
    send(gram.at[pl.ds(0, half)], gram_hbm.at[pl.ds(0, half)])
    gram[half:, :half] = b.T
    gram[half:, half:] = jnp.where(col < r, square, jnp.where(col == r, jnp.broadcast_to(last, (half, half)), turned))
    send(gram.at[pl.ds(half, half)], gram_hbm.at[pl.ds(half, half)])
    g_high, g_low = split(gram[...])
    both = dot(e_ref[...], g_high, 1, 0)
    train_ref[...] = (both[:m] + both[m:] + dot(e_ref[:m, :], g_low, 1, 0)) * scale_ref[:, :1]
    send(train_ref, train_hbm)
    for copy in sent:
        copy.wait()


def tail(packed, e_both, scales):
    m, k = scales.shape[0], e_both.shape[1]
    hbm, vmem = pl.BlockSpec(memory_space=pltpu.HBM), pl.BlockSpec(memory_space=pltpu.VMEM)
    coef = pltpu.HBM((m, k), F32)
    return pl.pallas_call(
        tail_kernel,
        out_shape=(pltpu.HBM((k, k), F32), coef, coef),
        in_specs=[vmem, vmem, vmem],
        out_specs=(hbm, hbm, hbm),
        scratch_shapes=[pltpu.VMEM((k, k), F32), pltpu.VMEM((m, k), F32), pltpu.SemaphoreType.DMA((k // LANES + 3,))],
        compiler_params=pltpu.CompilerParams(vmem_limit_bytes=16 * 1024 * 1024),
        name="tail",
    )(packed, e_both, scales)


def partners(n, r):
    return [(i, i ^ r) for i in range(n)]


def tree(parts):
    while len(parts) > 1:
        parts = [a + b for a, b in zip(parts[::2], parts[1::2], strict=True)]
    return parts[0]


def direct(n):
    return n <= DIRECT and n & (n - 1) == 0


def reduce_scatter(x, axis):
    n = lax.axis_size(axis)
    if not direct(n):
        return lax.psum_scatter(x, axis)
    me = lax.axis_index(axis)
    parts = [lax.dynamic_index_in_dim(x, me ^ r, 0, False) for r in range(n)]
    return tree([p if r == 0 else lax.ppermute(p, axis, partners(n, r)) for r, p in enumerate(parts)])


def all_reduce(x, axis):
    n = lax.axis_size(axis)
    if not direct(n):
        return lax.psum(x, axis)
    return tree([x if r == 0 else lax.ppermute(x, axis, partners(n, r)) for r in range(n)])


def all_gather(own, outer, inner):
    no, ni = lax.axis_size(outer), lax.axis_size(inner)
    if not (direct(no) and direct(ni)):
        return lax.all_gather(lax.all_gather(own, inner), outer)
    mo, mi = lax.axis_index(outer), lax.axis_index(inner)
    got = [own if r == 0 else lax.ppermute(own, inner, partners(ni, r)) for r in range(ni)]
    out = jnp.zeros((no, ni) + own.shape, own.dtype)
    for r, row in enumerate(got):
        for q in range(no):
            there = row if q == 0 else lax.ppermute(row, outer, partners(no, q))
            out = lax.dynamic_update_slice(out, there[None, None], (mo ^ q, mi ^ r) + (0,) * own.ndim)
    return out


def body(snapshots, validation, eigenvectors, eigenvalues):
    cores, chips = lax.axis_size("core"), lax.axis_size("chip")
    devices = cores * chips * lax.axis_size("plane")
    total = snapshots.shape[0] * devices * 1.0
    k, m = eigenvectors.shape
    piece = -(-layout(k, m)[-1] // (cores * chips * 8)) * 8
    e_rows, w_row = eigenvectors.T, eigenvalues[None, :]

    packed, modes, e_both, scales = head(snapshots, validation, e_rows, w_row, total, cores * chips * piece)
    own = reduce_scatter(packed.reshape(cores, chips, piece, LANES), "core")
    own = reduce_scatter(own, "chip")
    own = all_reduce(own, "plane")
    packed = all_gather(own, "core", "chip").reshape(-1, LANES)
    gram, train_coef, valid_coef = tail(packed, e_both, scales)
    return gram, modes, train_coef, valid_coef


def solution(mesh):
    inner = axes_of(mesh)
    rows = ("plane", "chip", "core")
    in_specs = (P(rows, None), P(rows, None), P(), P())
    out_specs = (P(), P(None, rows), P(), P())
    return jax.shard_map(body, mesh=inner, in_specs=in_specs, out_specs=out_specs, check_vma=False)
```

```python
import functools

import jax
import jax.numpy as jnp
from jax import lax
from jax.experimental import pallas as pl
from jax.experimental.pallas import tpu as pltpu
from jax.sharding import Mesh, PartitionSpec as P


LANES = 128
DIRECT = 4
F32 = jnp.float32


def axes_of(mesh):
    devices = list(mesh.devices.flat)
    cores = len({d.core_on_chip for d in devices})
    planes = len({d.coords[2] for d in devices})
    chips = len(devices) // (cores * planes)
    return Mesh(mesh.devices.reshape(planes, chips, cores), ("plane", "chip", "core"))


def layout(k, m):
    half = k // 2
    square = half * half // LANES
    mixed, cross, valid = 0, square, 2 * square
    diagonal = valid + m * k // LANES
    return mixed, cross, valid, diagonal, diagonal + half // LANES


def split(x):
    high = x.astype(jnp.bfloat16)
    return high, (x - high.astype(F32)).astype(jnp.bfloat16)


def dot(a, b, ca, cb):
    return lax.dot_general(a, b, (((ca,), (cb,)), ((), ())), preferred_element_type=F32)


def column(row, m):
    r, c = (lax.broadcasted_iota(jnp.int32, (m, m), d) for d in (0, 1))
    return jnp.sum(jnp.where(r == c, jnp.broadcast_to(row, (m, m)), 0.0), axis=1, keepdims=True)


def order(half):
    r, c = (lax.broadcasted_iota(jnp.int32, (half, half), d) for d in (0, 1))
    return r, c


def head_kernel(
    total, s_hbm, v_hbm, e_hbm, w_hbm, packed_ref, modes_hbm, e_out, scale_out, s_buf, v_buf, e_buf, w_buf, modes_ref, sems
):
    n, k = s_buf.shape
    m = e_buf.shape[0]
    half, step = k // 2, n // 2
    mixed, cross, valid, diagonal, _ = layout(k, m)
    copies = []
    halves = [pl.ds(i * step, step) for i in range(2)]
    for src, buf in [
        *((s_hbm.at[at], s_buf.at[at]) for at in halves), (e_hbm, e_buf), (w_hbm, w_buf),
        *((v_hbm.at[at], v_buf.at[at]) for at in halves),
    ]:
        copies.append(pltpu.make_async_copy(src, buf, sems.at[len(copies)]))
        copies[-1].start()
    a = b = c = None
    modes = []
    for i in range(2):
        copies[i].wait()
        high, low = split(s_buf[i * step : (i + 1) * step, :])
        ha, hb, la, lb = high[:, :half], high[:, half:], low[:, :half], low[:, half:]
        da = dot(ha, ha, 0, 0) + dot(ha, la, 0, 0) + dot(la, ha, 0, 0)
        db = dot(ha, hb, 0, 0) + dot(ha, lb, 0, 0) + dot(la, hb, 0, 0)
        dc = dot(hb, hb, 0, 0) + dot(hb, lb, 0, 0) + dot(lb, hb, 0, 0)
        a, b, c = (da, db, dc) if i == 0 else (a + da, b + db, c + dc)
        if i == 0:
            copies[2].wait()
            copies[3].wait()
            scales = column(lax.rsqrt(w_buf[...]), m)
            e_high, e_low = split(e_buf[...])
            e_both = jnp.concatenate([e_high, e_low], 0)
            e_out[...] = e_both
            scale_out[...] = jnp.broadcast_to(scales, scale_out.shape)
        both = dot(e_both, high, 1, 1)
        modes.append((both[:m] + both[m:] + dot(e_high, low, 1, 1)) * scales)
        modes_ref[:, i * step : (i + 1) * step] = modes[i]
    modes_out = pltpu.make_async_copy(modes_ref, modes_hbm, sems.at[6])
    modes_out.start()
    r, col = order(half)
    square = jnp.where(col >= r, a, c) * (1.0 / total)
    b = b * (1.0 / total)
    last = jnp.sum(jnp.where(col == r, c, 0.0), axis=0, keepdims=True) * (1.0 / total)
    for j in range(half // LANES):
        lanes = slice(j * LANES, (j + 1) * LANES)
        packed_ref[mixed + j * half : mixed + (j + 1) * half, :] = square[:, lanes]
        packed_ref[cross + j * half : cross + (j + 1) * half, :] = b[:, lanes]
    pad = packed_ref.shape[0] - diagonal
    packed_ref[diagonal:, :] = jnp.concatenate(
        [last[:, j * LANES : (j + 1) * LANES] for j in range(half // LANES)]
        + [jnp.zeros((pad - half // LANES, LANES), F32)], 0
    )
    out = None
    for i in range(2):
        copies[4 + i].wait()
        m_high, m_low = split(modes[i])
        v_high, v_low = split(v_buf[i * step : (i + 1) * step, :])
        both = dot(jnp.concatenate([m_high, m_low], 0), v_high, 1, 0)
        part = both[:m] + both[m:] + dot(m_high, v_low, 1, 0)
        out = part if i == 0 else out + part
    out = out * (1.0 / total)
    for j in range(k // LANES):
        packed_ref[valid + j * m : valid + (j + 1) * m, :] = out[:, j * LANES : (j + 1) * LANES]
    modes_out.wait()


def in_hbm(x):
    return pltpu.with_memory_space_constraint(x, pltpu.HBM)


def head(snapshots, validation, e_rows, w_row, total, rows):
    n, k = snapshots.shape
    m = e_rows.shape[0]
    hbm, vmem = pl.BlockSpec(memory_space=pltpu.HBM), pl.BlockSpec(memory_space=pltpu.VMEM)
    return pl.pallas_call(
        functools.partial(head_kernel, total),
        out_shape=(
            pltpu.VMEM((rows, LANES), F32), pltpu.HBM((m, n), F32),
            pltpu.VMEM((2 * m, k), jnp.bfloat16), pltpu.VMEM((m, LANES), F32),
        ),
        in_specs=[hbm] * 4,
        out_specs=(vmem, hbm, vmem, vmem),
        scratch_shapes=[
            pltpu.VMEM((n, k), F32), pltpu.VMEM((n, k), F32), pltpu.VMEM((m, k), F32), pltpu.VMEM((1, m), F32),
            pltpu.VMEM((m, n), F32), pltpu.SemaphoreType.DMA((7,)),
        ],
        compiler_params=pltpu.CompilerParams(vmem_limit_bytes=24 * 1024 * 1024),
        name="head",
    )(in_hbm(snapshots), in_hbm(validation), in_hbm(e_rows), in_hbm(w_row))


def tail_kernel(packed_ref, e_ref, scale_ref, gram_hbm, train_hbm, valid_hbm, gram, train_ref, sems):
    m, k = train_ref.shape
    half = k // 2
    mixed, cross, valid, diagonal, _ = layout(k, m)
    tiles = half // LANES
    sent = []

    def send(src, dst):
        sent.append(pltpu.make_async_copy(src, dst, sems.at[len(sent)]))
        sent[-1].start()

    for j in range(k // LANES):
        send(packed_ref.at[pl.ds(valid + j * m, m)], valid_hbm.at[:, pl.ds(j * LANES, LANES)])
    get = lambda first, j: packed_ref[first + j * half : first + (j + 1) * half, :]
    square = jnp.concatenate([get(mixed, j) for j in range(tiles)], 1)
    b = jnp.concatenate([get(cross, j) for j in range(tiles)], 1)
    last = jnp.concatenate([packed_ref[diagonal + j : diagonal + j + 1, :] for j in range(tiles)], 1)
    r, col = order(half)
    turned = square.T
    gram[:half, :half] = jnp.where(col >= r, square, turned)
    gram[:half, half:] = b
    send(gram.at[pl.ds(0, half)], gram_hbm.at[pl.ds(0, half)])
    gram[half:, :half] = b.T
    gram[half:, half:] = jnp.where(col < r, square, jnp.where(col == r, jnp.broadcast_to(last, (half, half)), turned))
    send(gram.at[pl.ds(half, half)], gram_hbm.at[pl.ds(half, half)])
    g_high, g_low = split(gram[...])
    both = dot(e_ref[...], g_high, 1, 0)
    train_ref[...] = (both[:m] + both[m:] + dot(e_ref[:m, :], g_low, 1, 0)) * scale_ref[:, :1]
    send(train_ref, train_hbm)
    for copy in sent:
        copy.wait()


def tail(packed, e_both, scales):
    m, k = scales.shape[0], e_both.shape[1]
    hbm, vmem = pl.BlockSpec(memory_space=pltpu.HBM), pl.BlockSpec(memory_space=pltpu.VMEM)
    coef = pltpu.HBM((m, k), F32)
    return pl.pallas_call(
        tail_kernel,
        out_shape=(pltpu.HBM((k, k), F32), coef, coef),
        in_specs=[vmem, vmem, vmem],
        out_specs=(hbm, hbm, hbm),
        scratch_shapes=[pltpu.VMEM((k, k), F32), pltpu.VMEM((m, k), F32), pltpu.SemaphoreType.DMA((k // LANES + 3,))],
        compiler_params=pltpu.CompilerParams(vmem_limit_bytes=16 * 1024 * 1024),
        name="tail",
    )(packed, e_both, scales)


def partners(n, r):
    return [(i, i ^ r) for i in range(n)]


def tree(parts):
    while len(parts) > 1:
        parts = [a + b for a, b in zip(parts[::2], parts[1::2], strict=True)]
    return parts[0]


def direct(n):
    return n <= DIRECT and n & (n - 1) == 0


def permute(x, axis, r):
    return lax.ppermute(x, axis, partners(lax.axis_size(axis), r))


def reduce_scatter(x, axis):
    n = lax.axis_size(axis)
    if not direct(n):
        return lax.psum_scatter(x, axis)
    me = lax.axis_index(axis)
    parts = [lax.dynamic_index_in_dim(x, me ^ r, 0, False) for r in range(n)]
    return tree([p if r == 0 else permute(p, axis, r) for r, p in enumerate(parts)])


def all_reduce(x, axis):
    n = lax.axis_size(axis)
    if not direct(n):
        return lax.psum(x, axis)
    return tree([x if r == 0 else permute(x, axis, r) for r in range(n)])


def all_gather(own, outer, inner):
    no, ni = lax.axis_size(outer), lax.axis_size(inner)
    if not (direct(no) and direct(ni)):
        return lax.all_gather(lax.all_gather(own, inner), outer)
    mo, mi = lax.axis_index(outer), lax.axis_index(inner)
    got = [own if r == 0 else permute(own, inner, r) for r in range(ni)]
    out = jnp.zeros((no, ni) + own.shape, own.dtype)
    for r, row in enumerate(got):
        for q in range(no):
            there = row if q == 0 else lax.ppermute(row, outer, partners(no, q))
            out = lax.dynamic_update_slice(out, there[None, None], (mo ^ q, mi ^ r) + (0,) * own.ndim)
    return out


def body(snapshots, validation, eigenvectors, eigenvalues):
    cores, chips = lax.axis_size("core"), lax.axis_size("chip")
    devices = cores * chips * lax.axis_size("plane")
    total = snapshots.shape[0] * devices * 1.0
    k, m = eigenvectors.shape
    piece = -(-layout(k, m)[-1] // (cores * chips * 8)) * 8
    e_rows, w_row = eigenvectors.T, eigenvalues[None, :]

    packed, modes, e_both, scales = head(snapshots, validation, e_rows, w_row, total, cores * chips * piece)
    own = reduce_scatter(packed.reshape(cores, chips, piece, LANES), "core")
    own = reduce_scatter(own, "chip")
    own = all_reduce(own, "plane")
    packed = all_gather(own, "core", "chip").reshape(-1, LANES)
    gram, train_coef, valid_coef = tail(packed, e_both, scales)
    return gram, modes, train_coef, valid_coef


def solution(mesh):
    inner = axes_of(mesh)
    rows = ("plane", "chip", "core")
    in_specs = (P(rows, None), P(rows, None), P(), P())
    out_specs = (P(), P(None, rows), P(), P())
    step = jax.shard_map(body, mesh=inner, in_specs=in_specs, out_specs=out_specs, check_vma=False)
    if not all(direct(n) for n in inner.devices.shape):
        return step
    return step
```

```python
import functools

import jax
import jax.numpy as jnp
from jax import lax
from jax.experimental import pallas as pl
from jax.experimental.pallas import tpu as pltpu
from jax.sharding import Mesh, PartitionSpec as P


LANES = 128
DIRECT = 4
F32 = jnp.float32


def axes_of(mesh):
    devices = list(mesh.devices.flat)
    cores = len({d.core_on_chip for d in devices})
    planes = len({d.coords[2] for d in devices})
    chips = len(devices) // (cores * planes)
    return Mesh(mesh.devices.reshape(planes, chips, cores), ("plane", "chip", "core"))


def layout(k, m):
    half = k // 2
    square = half * half // LANES
    mixed, cross, valid = 0, square, 2 * square
    diagonal = valid + m * k // LANES
    return mixed, cross, valid, diagonal, diagonal + half // LANES


def split(x):
    high = x.astype(jnp.bfloat16)
    return high, (x - high.astype(F32)).astype(jnp.bfloat16)


def dot(a, b, ca, cb):
    return lax.dot_general(a, b, (((ca,), (cb,)), ((), ())), preferred_element_type=F32)


def column(row, m):
    r, c = (lax.broadcasted_iota(jnp.int32, (m, m), d) for d in (0, 1))
    return jnp.sum(jnp.where(r == c, jnp.broadcast_to(row, (m, m)), 0.0), axis=1, keepdims=True)


def order(half):
    r, c = (lax.broadcasted_iota(jnp.int32, (half, half), d) for d in (0, 1))
    return r, c


def head_kernel(
    total, s_hbm, v_hbm, e_hbm, w_hbm, packed_ref, modes_ref, e_out, scale_out, s_buf, v_buf, e_buf, w_buf, sems
):
    _, k = s_buf.shape
    m = e_buf.shape[0]
    half = k // 2
    mixed, cross, valid, diagonal, _ = layout(k, m)
    copies = []
    for src, buf in [(e_hbm, e_buf), (w_hbm, w_buf), (s_hbm, s_buf), (v_hbm, v_buf)]:
        copies.append(pltpu.make_async_copy(src, buf, sems.at[len(copies)]))
        copies[-1].start()
    for copy in copies[:2]:
        copy.wait()
    scales = column(lax.rsqrt(w_buf[...]), m)
    e_high, e_low = split(e_buf[...])
    e_both = jnp.concatenate([e_high, e_low], 0)
    e_out[...] = e_both
    scale_out[...] = jnp.broadcast_to(scales, scale_out.shape)
    for copy in copies[2:]:
        copy.wait()
    high, low = split(s_buf[...])
    both = dot(high, e_both, 1, 1)
    modes = (both[:, :m] + both[:, m:] + dot(low, e_high, 1, 1)).T * scales
    modes_ref[...] = modes
    ha, hb, la, lb = high[:, :half], high[:, half:], low[:, :half], low[:, half:]
    xa, xb, xc = dot(ha, la, 0, 0), dot(hb, la, 0, 0), dot(hb, lb, 0, 0)
    a = dot(ha, ha, 0, 0) + (xa + xa.T)
    b = dot(ha, hb, 0, 0) + (dot(ha, lb, 0, 0) + xb.T)
    c = dot(hb, hb, 0, 0) + (xc + xc.T)
    m_high, m_low = split(modes)
    v_high, v_low = split(v_buf[...])
    both = dot(jnp.concatenate([m_high, m_low], 0), v_high, 1, 0)
    out = (both[:m] + both[m:] + dot(m_high, v_low, 1, 0)) * (1.0 / total)
    r, col = order(half)
    square = jnp.where(col >= r, a, c) * (1.0 / total)
    b = b * (1.0 / total)
    last = jnp.sum(jnp.where(col == r, c, 0.0), axis=0, keepdims=True) * (1.0 / total)
    for j in range(half // LANES):
        lanes = slice(j * LANES, (j + 1) * LANES)
        packed_ref[mixed + j * half : mixed + (j + 1) * half, :] = square[:, lanes]
        packed_ref[cross + j * half : cross + (j + 1) * half, :] = b[:, lanes]
    pad = packed_ref.shape[0] - diagonal
    packed_ref[diagonal:, :] = jnp.concatenate(
        [last[:, j * LANES : (j + 1) * LANES] for j in range(half // LANES)]
        + [jnp.zeros((pad - half // LANES, LANES), F32)], 0
    )
    for j in range(k // LANES):
        packed_ref[valid + j * m : valid + (j + 1) * m, :] = out[:, j * LANES : (j + 1) * LANES]


def in_hbm(x):
    return pltpu.with_memory_space_constraint(x, pltpu.HBM)


def head(snapshots, validation, e_rows, w_row, total, rows):
    n, k = snapshots.shape
    m = e_rows.shape[0]
    hbm, vmem = pl.BlockSpec(memory_space=pltpu.HBM), pl.BlockSpec(memory_space=pltpu.VMEM)
    return pl.pallas_call(
        functools.partial(head_kernel, total),
        out_shape=(
            pltpu.VMEM((rows, LANES), F32), pltpu.VMEM((m, n), F32),
            pltpu.VMEM((2 * m, k), jnp.bfloat16), pltpu.VMEM((m, LANES), F32),
        ),
        in_specs=[hbm] * 4,
        out_specs=(vmem,) * 4,
        scratch_shapes=[
            pltpu.VMEM((n, k), F32), pltpu.VMEM((n, k), F32), pltpu.VMEM((m, k), F32), pltpu.VMEM((1, m), F32),
            pltpu.SemaphoreType.DMA((4,)),
        ],
        compiler_params=pltpu.CompilerParams(vmem_limit_bytes=24 * 1024 * 1024),
        name="head",
    )(in_hbm(snapshots), in_hbm(validation), in_hbm(e_rows), in_hbm(w_row))


def tail_kernel(
    packed_ref, modes_ref, e_ref, scale_ref, gram_hbm, modes_hbm, train_hbm, valid_hbm, gram, train_ref, sems
):
    m, k = train_ref.shape
    half = k // 2
    mixed, cross, valid, diagonal, _ = layout(k, m)
    tiles = half // LANES
    first, second = pl.ds(0, half), pl.ds(half, half)
    sent = []

    def send(src, dst):
        sent.append(pltpu.make_async_copy(src, dst, sems.at[len(sent)]))
        sent[-1].start()

    for j in range(tiles):
        at = pl.ds(half + j * LANES, LANES)
        send(packed_ref.at[pl.ds(cross + j * half, half)], gram_hbm.at[first, at])
    get = lambda start, j: packed_ref[start + j * half : start + (j + 1) * half, :]
    square = jnp.concatenate([get(mixed, j) for j in range(tiles)], 1)
    r, col = order(half)
    turned = square.T
    gram[:half, :half] = jnp.where(col >= r, square, turned)
    send(gram.at[first, first], gram_hbm.at[first, first])
    last = jnp.concatenate([packed_ref[diagonal + j : diagonal + j + 1, :] for j in range(tiles)], 1)
    gram[half:, half:] = jnp.where(col < r, square, jnp.where(col == r, jnp.broadcast_to(last, (half, half)), turned))
    send(gram.at[second, second], gram_hbm.at[second, second])
    b = jnp.concatenate([get(cross, j) for j in range(tiles)], 1)
    gram[half:, :half] = b.T
    send(gram.at[second, first], gram_hbm.at[second, first])
    gram[:half, half:] = b
    send(modes_ref, modes_hbm)
    for j in range(k // LANES):
        send(packed_ref.at[pl.ds(valid + j * m, m)], valid_hbm.at[:, pl.ds(j * LANES, LANES)])
    g_high, g_low = split(gram[...])
    both = dot(e_ref[...], g_high, 1, 0)
    train_ref[...] = (both[:m] + both[m:] + dot(e_ref[:m, :], g_low, 1, 0)) * scale_ref[:, :1]
    send(train_ref, train_hbm)
    for copy in sent:
        copy.wait()


def tail(packed, modes, e_both, scales):
    m, k = scales.shape[0], e_both.shape[1]
    hbm, vmem = pl.BlockSpec(memory_space=pltpu.HBM), pl.BlockSpec(memory_space=pltpu.VMEM)
    coef = pltpu.HBM((m, k), F32)
    return pl.pallas_call(
        tail_kernel,
        out_shape=(pltpu.HBM((k, k), F32), pltpu.HBM(modes.shape, F32), coef, coef),
        in_specs=[vmem] * 4,
        out_specs=(hbm,) * 4,
        scratch_shapes=[pltpu.VMEM((k, k), F32), pltpu.VMEM((m, k), F32), pltpu.SemaphoreType.DMA((3 * k // (2 * LANES) + 5,))],
        compiler_params=pltpu.CompilerParams(vmem_limit_bytes=16 * 1024 * 1024),
        name="tail",
    )(packed, modes, e_both, scales)


def partners(n, r):
    return [(i, i ^ r) for i in range(n)]


def tree(parts):
    while len(parts) > 1:
        parts = [a + b for a, b in zip(parts[::2], parts[1::2], strict=True)]
    return parts[0]


def direct(n):
    return n <= DIRECT and n & (n - 1) == 0


def permute(x, axis, r):
    return lax.ppermute(x, axis, partners(lax.axis_size(axis), r))


def reduce_scatter(x):
    cores, chips = x.shape[:2]
    if not (cores == 2 and chips > 1 and direct(chips)):
        return lax.psum_scatter(lax.psum_scatter(x, "core"), "chip")
    core, chip = lax.axis_index("core"), lax.axis_index("chip")
    row = lambda c, r: lax.dynamic_slice(x, (c, chip ^ r) + (0,) * (x.ndim - 2), (1, 1) + x.shape[2:])[0, 0]
    up = lambda rows: permute(jnp.stack([row(1 - core, r) for r in rows]), "core", 1)
    first = row(core, 1) + up([1])[0]
    others = [r for r in range(chips) if r != 1]
    theirs, _ = lax.optimization_barrier((up(others), first))
    parts = [row(core, r) + theirs[i] for i, r in enumerate(others)]
    parts.insert(1, first)
    return tree([p if r == 0 else permute(p, "chip", r) for r, p in enumerate(parts)])


def all_reduce(x, axis):
    n = lax.axis_size(axis)
    if not direct(n):
        return lax.psum(x, axis)
    return tree([x if r == 0 else permute(x, axis, r) for r in range(n)])


def all_gather(own, outer, inner):
    no, ni = lax.axis_size(outer), lax.axis_size(inner)
    if not (direct(no) and direct(ni)):
        return lax.all_gather(lax.all_gather(own, inner), outer)
    mo, mi = lax.axis_index(outer), lax.axis_index(inner)
    got = [own if r == 0 else permute(own, inner, r) for r in range(ni)]
    out = jnp.zeros((no, ni) + own.shape, own.dtype)
    for r, row in enumerate(got):
        for q in range(no):
            there = row if q == 0 else lax.ppermute(row, outer, partners(no, q))
            out = lax.dynamic_update_slice(out, there[None, None], (mo ^ q, mi ^ r) + (0,) * own.ndim)
    return out


def body(snapshots, validation, eigenvectors, eigenvalues):
    cores, chips = lax.axis_size("core"), lax.axis_size("chip")
    devices = cores * chips * lax.axis_size("plane")
    total = snapshots.shape[0] * devices * 1.0
    k, m = eigenvectors.shape
    piece = -(-layout(k, m)[-1] // (cores * chips * 8)) * 8
    e_rows, w_row = eigenvectors.T, eigenvalues[None, :]

    packed, modes, e_both, scales = head(snapshots, validation, e_rows, w_row, total, cores * chips * piece)
    own = reduce_scatter(packed.reshape(cores, chips, piece, LANES))
    own = all_reduce(own, "plane")
    packed = all_gather(own, "core", "chip").reshape(-1, LANES)
    return tail(packed, modes, e_both, scales)


def solution(mesh):
    inner = axes_of(mesh)
    rows = ("plane", "chip", "core")
    in_specs = (P(rows, None), P(rows, None), P(), P())
    out_specs = (P(), P(None, rows), P(), P())
    step = jax.shard_map(body, mesh=inner, in_specs=in_specs, out_specs=out_specs, check_vma=False)
    if not all(direct(n) for n in inner.devices.shape):
        return step
    return step
```

```python
import functools

import jax
import jax.numpy as jnp
from jax import lax
from jax.experimental import pallas as pl
from jax.experimental.pallas import tpu as pltpu
from jax.sharding import Mesh, PartitionSpec as P


LANES = 128
DIRECT = 4
F32 = jnp.float32


def axes_of(mesh):
    devices = list(mesh.devices.flat)
    cores = len({d.core_on_chip for d in devices})
    planes = len({d.coords[2] for d in devices})
    chips = len(devices) // (cores * planes)
    return Mesh(mesh.devices.reshape(planes, chips, cores), ("plane", "chip", "core"))


def layout(k, m):
    half = k // 2
    square = half * half // LANES
    mixed, cross, valid = 0, square, 2 * square
    diagonal = valid + m * k // LANES
    return mixed, cross, valid, diagonal, diagonal + half // LANES


def split(x):
    high = x.astype(jnp.bfloat16)
    return high, (x - high.astype(F32)).astype(jnp.bfloat16)


def dot(a, b, ca, cb):
    return lax.dot_general(a, b, (((ca,), (cb,)), ((), ())), preferred_element_type=F32)


def column(row, m):
    r, c = (lax.broadcasted_iota(jnp.int32, (m, m), d) for d in (0, 1))
    return jnp.sum(jnp.where(r == c, jnp.broadcast_to(row, (m, m)), 0.0), axis=1, keepdims=True)


def order(half):
    r, c = (lax.broadcasted_iota(jnp.int32, (half, half), d) for d in (0, 1))
    return r, c


def head_kernel(
    total, s_hbm, v_hbm, e_hbm, w_hbm, packed_ref, modes_ref, e_out, scale_out, s_buf, v_buf, e_buf, w_buf, sems
):
    _, k = s_buf.shape
    m = e_buf.shape[0]
    half = k // 2
    mixed, cross, valid, diagonal, _ = layout(k, m)
    copies = []
    for src, buf in [(e_hbm, e_buf), (w_hbm, w_buf), (s_hbm, s_buf), (v_hbm, v_buf)]:
        copies.append(pltpu.make_async_copy(src, buf, sems.at[len(copies)]))
        copies[-1].start()
    for copy in copies[:2]:
        copy.wait()
    scales = column(lax.rsqrt(w_buf[...]), m)
    e_high, e_low = split(e_buf[...])
    e_both = jnp.concatenate([e_high, e_low], 0)
    e_out[...] = e_both
    scale_out[...] = jnp.broadcast_to(scales, scale_out.shape)
    for copy in copies[2:]:
        copy.wait()
    high, low = split(s_buf[...])
    both = dot(high, e_both, 1, 1)
    modes = (both[:, :m] + both[:, m:] + dot(low, e_high, 1, 1)).T * scales
    modes_ref[...] = modes
    ha, hb, la, lb = high[:, :half], high[:, half:], low[:, :half], low[:, half:]
    xa, xb, xc = dot(ha, la, 0, 0), dot(hb, la, 0, 0), dot(hb, lb, 0, 0)
    a = dot(ha, ha, 0, 0) + (xa + xa.T)
    b = dot(ha, hb, 0, 0) + (dot(ha, lb, 0, 0) + xb.T)
    c = dot(hb, hb, 0, 0) + (xc + xc.T)
    m_high, m_low = split(modes)
    v_high, v_low = split(v_buf[...])
    both = dot(jnp.concatenate([m_high, m_low], 0), v_high, 1, 0)
    out = (both[:m] + both[m:] + dot(m_high, v_low, 1, 0)) * (1.0 / total)
    r, col = order(half)
    square = jnp.where(col >= r, a, c) * (1.0 / total)
    b = b * (1.0 / total)
    last = jnp.sum(jnp.where(col == r, c, 0.0), axis=0, keepdims=True) * (1.0 / total)
    for j in range(half // LANES):
        lanes = slice(j * LANES, (j + 1) * LANES)
        packed_ref[mixed + j * half : mixed + (j + 1) * half, :] = square[:, lanes]
        packed_ref[cross + j * half : cross + (j + 1) * half, :] = b[:, lanes]
    pad = packed_ref.shape[0] - diagonal
    packed_ref[diagonal:, :] = jnp.concatenate(
        [last[:, j * LANES : (j + 1) * LANES] for j in range(half // LANES)]
        + [jnp.zeros((pad - half // LANES, LANES), F32)], 0
    )
    for j in range(k // LANES):
        packed_ref[valid + j * m : valid + (j + 1) * m, :] = out[:, j * LANES : (j + 1) * LANES]


def in_hbm(x):
    return pltpu.with_memory_space_constraint(x, pltpu.HBM)


def head(snapshots, validation, e_rows, w_row, total, rows):
    n, k = snapshots.shape
    m = e_rows.shape[0]
    hbm, vmem = pl.BlockSpec(memory_space=pltpu.HBM), pl.BlockSpec(memory_space=pltpu.VMEM)
    return pl.pallas_call(
        functools.partial(head_kernel, total),
        out_shape=(
            pltpu.VMEM((rows, LANES), F32), pltpu.VMEM((m, n), F32),
            pltpu.VMEM((2 * m, k), jnp.bfloat16), pltpu.VMEM((m, LANES), F32),
        ),
        in_specs=[hbm] * 4,
        out_specs=(vmem,) * 4,
        scratch_shapes=[
            pltpu.VMEM((n, k), F32), pltpu.VMEM((n, k), F32), pltpu.VMEM((m, k), F32), pltpu.VMEM((1, m), F32),
            pltpu.SemaphoreType.DMA((4,)),
        ],
        compiler_params=pltpu.CompilerParams(vmem_limit_bytes=24 * 1024 * 1024),
        name="head",
    )(in_hbm(snapshots), in_hbm(validation), in_hbm(e_rows), in_hbm(w_row))


def tail_kernel(
    packed_ref, e_ref, scale_ref, gram_hbm, train_hbm, valid_hbm, gram, train_ref, sems
):
    m, k = train_ref.shape
    half = k // 2
    mixed, cross, valid, diagonal, _ = layout(k, m)
    tiles = half // LANES
    first, second = pl.ds(0, half), pl.ds(half, half)
    sent = []

    def send(src, dst):
        sent.append(pltpu.make_async_copy(src, dst, sems.at[len(sent)]))
        sent[-1].start()

    for j in range(tiles):
        at = pl.ds(half + j * LANES, LANES)
        send(packed_ref.at[pl.ds(cross + j * half, half)], gram_hbm.at[first, at])
    get = lambda start, j: packed_ref[start + j * half : start + (j + 1) * half, :]
    square = jnp.concatenate([get(mixed, j) for j in range(tiles)], 1)
    r, col = order(half)
    turned = square.T
    gram[:half, :half] = jnp.where(col >= r, square, turned)
    send(gram.at[first, first], gram_hbm.at[first, first])
    last = jnp.concatenate([packed_ref[diagonal + j : diagonal + j + 1, :] for j in range(tiles)], 1)
    gram[half:, half:] = jnp.where(col < r, square, jnp.where(col == r, jnp.broadcast_to(last, (half, half)), turned))
    send(gram.at[second, second], gram_hbm.at[second, second])
    b = jnp.concatenate([get(cross, j) for j in range(tiles)], 1)
    gram[half:, :half] = b.T
    send(gram.at[second, first], gram_hbm.at[second, first])
    gram[:half, half:] = b
    for j in range(k // LANES):
        send(packed_ref.at[pl.ds(valid + j * m, m)], valid_hbm.at[:, pl.ds(j * LANES, LANES)])
    g_high, g_low = split(gram[...])
    both = dot(e_ref[...], g_high, 1, 0)
    train_ref[...] = (both[:m] + both[m:] + dot(e_ref[:m, :], g_low, 1, 0)) * scale_ref[:, :1]
    send(train_ref, train_hbm)
    for copy in sent:
        copy.wait()


def tail(packed, e_both, scales):
    m, k = scales.shape[0], e_both.shape[1]
    hbm, vmem = pl.BlockSpec(memory_space=pltpu.HBM), pl.BlockSpec(memory_space=pltpu.VMEM)
    coef = pltpu.HBM((m, k), F32)
    return pl.pallas_call(
        tail_kernel,
        out_shape=(pltpu.HBM((k, k), F32), coef, coef),
        in_specs=[vmem] * 3,
        out_specs=(hbm,) * 3,
        scratch_shapes=[pltpu.VMEM((k, k), F32), pltpu.VMEM((m, k), F32), pltpu.SemaphoreType.DMA((3 * k // (2 * LANES) + 4,))],
        compiler_params=pltpu.CompilerParams(vmem_limit_bytes=16 * 1024 * 1024),
        name="tail",
    )(packed, e_both, scales)


def partners(n, r):
    return [(i, i ^ r) for i in range(n)]


def tree(parts):
    while len(parts) > 1:
        parts = [a + b for a, b in zip(parts[::2], parts[1::2], strict=True)]
    return parts[0]


def direct(n):
    return n <= DIRECT and n & (n - 1) == 0


def permute(x, axis, r):
    return lax.ppermute(x, axis, partners(lax.axis_size(axis), r))


def reduce_scatter(x):
    cores, chips = x.shape[:2]
    if not (cores == 2 and chips > 1 and direct(chips)):
        return lax.psum_scatter(lax.psum_scatter(x, "core"), "chip")
    core, chip = lax.axis_index("core"), lax.axis_index("chip")
    row = lambda c, r: lax.dynamic_slice(x, (c, chip ^ r) + (0,) * (x.ndim - 2), (1, 1) + x.shape[2:])[0, 0]
    up = lambda rows: permute(jnp.stack([row(1 - core, r) for r in rows]), "core", 1)
    first = row(core, 1) + up([1])[0]
    others = [r for r in range(chips) if r != 1]
    theirs, _ = lax.optimization_barrier((up(others), first))
    parts = [row(core, r) + theirs[i] for i, r in enumerate(others)]
    parts.insert(1, first)
    return tree([p if r == 0 else permute(p, "chip", r) for r, p in enumerate(parts)])


def all_reduce(x, axis):
    n = lax.axis_size(axis)
    if not direct(n):
        return lax.psum(x, axis)
    return tree([x if r == 0 else permute(x, axis, r) for r in range(n)])


def all_gather(own, outer, inner):
    no, ni = lax.axis_size(outer), lax.axis_size(inner)
    if not (direct(no) and direct(ni)):
        return lax.all_gather(lax.all_gather(own, inner), outer)
    mo, mi = lax.axis_index(outer), lax.axis_index(inner)
    got = [own if r == 0 else permute(own, inner, r) for r in range(ni)]
    out = jnp.zeros((no, ni) + own.shape, own.dtype)
    for r, row in enumerate(got):
        for q in range(no):
            there = row if q == 0 else lax.ppermute(row, outer, partners(no, q))
            out = lax.dynamic_update_slice(out, there[None, None], (mo ^ q, mi ^ r) + (0,) * own.ndim)
    return out


def body(snapshots, validation, eigenvectors, eigenvalues):
    cores, chips = lax.axis_size("core"), lax.axis_size("chip")
    devices = cores * chips * lax.axis_size("plane")
    total = snapshots.shape[0] * devices * 1.0
    k, m = eigenvectors.shape
    piece = -(-layout(k, m)[-1] // (cores * chips * 8)) * 8
    e_rows, w_row = eigenvectors.T, eigenvalues[None, :]

    packed, modes, e_both, scales = head(snapshots, validation, e_rows, w_row, total, cores * chips * piece)
    own = reduce_scatter(packed.reshape(cores, chips, piece, LANES))
    own = all_reduce(own, "plane")
    packed = all_gather(own, "core", "chip").reshape(-1, LANES)
    gram, train_coef, valid_coef = tail(packed, e_both, scales)
    return gram, modes, train_coef, valid_coef


def solution(mesh):
    inner = axes_of(mesh)
    rows = ("plane", "chip", "core")
    in_specs = (P(rows, None), P(rows, None), P(), P())
    out_specs = (P(), P(None, rows), P(), P())
    step = jax.shard_map(body, mesh=inner, in_specs=in_specs, out_specs=out_specs, check_vma=False)
    if not all(direct(n) for n in inner.devices.shape):
        return step
    return step
```

```python
import functools

import jax
import jax.numpy as jnp
from jax import lax
from jax.experimental import pallas as pl
from jax.experimental.pallas import tpu as pltpu
from jax.sharding import Mesh, PartitionSpec as P


LANES = 128
DIRECT = 4
F32 = jnp.float32
SCATTER = ((1, 1), (2, 2), (3, 3))
SPREAD = ((3, 3), (2, 1), (1, 2))


def axes_of(mesh):
    devices = list(mesh.devices.flat)
    cores = len({d.core_on_chip for d in devices})
    planes = len({d.coords[2] for d in devices})
    chips = len(devices) // (cores * planes)
    return Mesh(mesh.devices.reshape(planes, chips, cores), ("plane", "chip", "core"))


def layout(k, m):
    half = k // 2
    square = half * half // LANES
    mixed, cross, valid = 0, square, 2 * square
    diagonal = valid + m * k // LANES
    return mixed, cross, valid, diagonal, diagonal + half // LANES


def split(x):
    high = x.astype(jnp.bfloat16)
    return high, (x - high.astype(F32)).astype(jnp.bfloat16)


def dot(a, b, ca, cb):
    return lax.dot_general(a, b, (((ca,), (cb,)), ((), ())), preferred_element_type=F32)


def column(row, m):
    r, c = (lax.broadcasted_iota(jnp.int32, (m, m), d) for d in (0, 1))
    return jnp.sum(jnp.where(r == c, jnp.broadcast_to(row, (m, m)), 0.0), axis=1, keepdims=True)


def order(half):
    r, c = (lax.broadcasted_iota(jnp.int32, (half, half), d) for d in (0, 1))
    return r, c


def head_kernel(
    total, s_hbm, v_hbm, e_hbm, w_hbm, packed_ref, modes_ref, e_out, scale_out, s_buf, v_buf, e_buf, w_buf, sems
):
    _, k = s_buf.shape
    m = e_buf.shape[0]
    half = k // 2
    mixed, cross, valid, diagonal, _ = layout(k, m)
    copies = []
    for src, buf in [(e_hbm, e_buf), (w_hbm, w_buf), (s_hbm, s_buf), (v_hbm, v_buf)]:
        copies.append(pltpu.make_async_copy(src, buf, sems.at[len(copies)]))
        copies[-1].start()
    for copy in copies[:2]:
        copy.wait()
    scales = column(lax.rsqrt(w_buf[...]), m)
    e_high, e_low = split(e_buf[...])
    e_both = jnp.concatenate([e_high, e_low], 0)
    e_out[...] = e_both
    scale_out[...] = jnp.broadcast_to(scales, scale_out.shape)
    for copy in copies[2:]:
        copy.wait()
    high, low = split(s_buf[...])
    both = dot(high, e_both, 1, 1)
    modes = (both[:, :m] + both[:, m:] + dot(low, e_high, 1, 1)).T * scales
    modes_ref[...] = modes
    ha, hb, la, lb = high[:, :half], high[:, half:], low[:, :half], low[:, half:]
    xa, xb, xc = dot(ha, la, 0, 0), dot(hb, la, 0, 0), dot(hb, lb, 0, 0)
    a = dot(ha, ha, 0, 0) + (xa + xa.T)
    b = dot(ha, hb, 0, 0) + (dot(ha, lb, 0, 0) + xb.T)
    c = dot(hb, hb, 0, 0) + (xc + xc.T)
    m_high, m_low = split(modes)
    v_high, v_low = split(v_buf[...])
    both = dot(jnp.concatenate([m_high, m_low], 0), v_high, 1, 0)
    out = (both[:m] + both[m:] + dot(m_high, v_low, 1, 0)) * (1.0 / total)
    r, col = order(half)
    square = jnp.where(col >= r, a, c) * (1.0 / total)
    b = b * (1.0 / total)
    last = jnp.sum(jnp.where(col == r, c, 0.0), axis=0, keepdims=True) * (1.0 / total)
    for j in range(half // LANES):
        lanes = slice(j * LANES, (j + 1) * LANES)
        packed_ref[mixed + j * half : mixed + (j + 1) * half, :] = square[:, lanes]
        packed_ref[cross + j * half : cross + (j + 1) * half, :] = b[:, lanes]
    pad = packed_ref.shape[0] - diagonal
    packed_ref[diagonal:, :] = jnp.concatenate(
        [last[:, j * LANES : (j + 1) * LANES] for j in range(half // LANES)]
        + [jnp.zeros((pad - half // LANES, LANES), F32)], 0
    )
    for j in range(k // LANES):
        packed_ref[valid + j * m : valid + (j + 1) * m, :] = out[:, j * LANES : (j + 1) * LANES]


def in_hbm(x):
    return pltpu.with_memory_space_constraint(x, pltpu.HBM)


def head(snapshots, validation, e_rows, w_row, total, rows):
    n, k = snapshots.shape
    m = e_rows.shape[0]
    hbm, vmem = pl.BlockSpec(memory_space=pltpu.HBM), pl.BlockSpec(memory_space=pltpu.VMEM)
    return pl.pallas_call(
        functools.partial(head_kernel, total),
        out_shape=(
            pltpu.VMEM((rows, LANES), F32), pltpu.VMEM((m, n), F32),
            pltpu.VMEM((2 * m, k), jnp.bfloat16), pltpu.VMEM((m, LANES), F32),
        ),
        in_specs=[hbm] * 4,
        out_specs=(vmem,) * 4,
        scratch_shapes=[
            pltpu.VMEM((n, k), F32), pltpu.VMEM((n, k), F32), pltpu.VMEM((m, k), F32), pltpu.VMEM((1, m), F32),
            pltpu.SemaphoreType.DMA((4,)),
        ],
        compiler_params=pltpu.CompilerParams(vmem_limit_bytes=24 * 1024 * 1024),
        name="head",
    )(in_hbm(snapshots), in_hbm(validation), in_hbm(e_rows), in_hbm(w_row))


def tail_kernel(
    packed_ref, modes_ref, e_ref, scale_ref, gram_hbm, modes_hbm, train_hbm, valid_hbm, gram, train_ref, sems
):
    m, k = train_ref.shape
    half = k // 2
    mixed, cross, valid, diagonal, _ = layout(k, m)
    tiles = half // LANES
    first, second = pl.ds(0, half), pl.ds(half, half)
    sent = []

    def send(src, dst):
        sent.append(pltpu.make_async_copy(src, dst, sems.at[len(sent)]))
        sent[-1].start()

    for j in range(tiles):
        at = pl.ds(half + j * LANES, LANES)
        send(packed_ref.at[pl.ds(cross + j * half, half)], gram_hbm.at[first, at])
    get = lambda start, j: packed_ref[start + j * half : start + (j + 1) * half, :]
    square = jnp.concatenate([get(mixed, j) for j in range(tiles)], 1)
    r, col = order(half)
    turned = square.T
    gram[:half, :half] = jnp.where(col >= r, square, turned)
    send(gram.at[first, first], gram_hbm.at[first, first])
    last = jnp.concatenate([packed_ref[diagonal + j : diagonal + j + 1, :] for j in range(tiles)], 1)
    gram[half:, half:] = jnp.where(col < r, square, jnp.where(col == r, jnp.broadcast_to(last, (half, half)), turned))
    send(gram.at[second, second], gram_hbm.at[second, second])
    b = jnp.concatenate([get(cross, j) for j in range(tiles)], 1)
    gram[half:, :half] = b.T
    send(gram.at[second, first], gram_hbm.at[second, first])
    gram[:half, half:] = b
    send(modes_ref, modes_hbm)
    for j in range(k // LANES):
        send(packed_ref.at[pl.ds(valid + j * m, m)], valid_hbm.at[:, pl.ds(j * LANES, LANES)])
    g_high, g_low = split(gram[...])
    both = dot(e_ref[...], g_high, 1, 0)
    train_ref[...] = (both[:m] + both[m:] + dot(e_ref[:m, :], g_low, 1, 0)) * scale_ref[:, :1]
    send(train_ref, train_hbm)
    for copy in sent:
        copy.wait()


def tail(packed, modes, e_both, scales):
    m, k = scales.shape[0], e_both.shape[1]
    hbm, vmem = pl.BlockSpec(memory_space=pltpu.HBM), pl.BlockSpec(memory_space=pltpu.VMEM)
    coef = pltpu.HBM((m, k), F32)
    return pl.pallas_call(
        tail_kernel,
        out_shape=(pltpu.HBM((k, k), F32), pltpu.HBM(modes.shape, F32), coef, coef),
        in_specs=[vmem] * 4,
        out_specs=(hbm,) * 4,
        scratch_shapes=[pltpu.VMEM((k, k), F32), pltpu.VMEM((m, k), F32), pltpu.SemaphoreType.DMA((3 * k // (2 * LANES) + 5,))],
        compiler_params=pltpu.CompilerParams(vmem_limit_bytes=16 * 1024 * 1024),
        name="tail",
    )(packed, modes, e_both, scales)


def partners(n, r):
    return [(i, i ^ r) for i in range(n)]


def tree(parts):
    while len(parts) > 1:
        parts = [a + b for a, b in zip(parts[::2], parts[1::2], strict=True)]
    return parts[0]


def direct(n):
    return n <= DIRECT and n & (n - 1) == 0


def permute(x, axis, r):
    return lax.ppermute(x, axis, partners(lax.axis_size(axis), r))


def planar(cores, chips):
    return cores == 2 and chips == DIRECT


def reach(steps, core, i):
    return jnp.where(core == 0, steps[i][0], steps[i][1]) if i < len(steps) else 0


def swap(x, steps, i):
    pairs = [(2 * q + c, 2 * (q ^ steps[i][c]) + c) for q in range(DIRECT) for c in range(2)]
    return lax.ppermute(x, ("chip", "core"), pairs)


def reduce_scatter(x):
    cores, chips = x.shape[:2]
    if not planar(cores, chips):
        return lax.psum_scatter(lax.psum_scatter(x, "core"), "chip")
    core, chip = lax.axis_index("core"), lax.axis_index("chip")

    def row(c, i):
        return lax.dynamic_slice(x, (c, chip ^ reach(SCATTER, c, i)) + (0,) * (x.ndim - 2), (1, 1) + x.shape[2:])[0, 0]

    up = lambda rows: permute(jnp.stack([row(1 - core, r) for r in rows]), "core", 1)
    first = row(core, 0) + up([0])[0]
    theirs, _ = lax.optimization_barrier((up(range(1, chips)), first))
    parts = [first] + [row(core, i) + theirs[i - 1] for i in range(1, chips)]
    return tree([swap(p, SCATTER, i) if i < chips - 1 else p for i, p in enumerate(parts)])


def all_reduce(x, axis):
    n = lax.axis_size(axis)
    if not direct(n):
        return lax.psum(x, axis)
    return tree([x if r == 0 else permute(x, axis, r) for r in range(n)])


def all_gather(own):
    cores, chips = lax.axis_size("core"), lax.axis_size("chip")
    if not planar(cores, chips):
        return lax.all_gather(lax.all_gather(own, "chip"), "core")
    core, chip = lax.axis_index("core"), lax.axis_index("chip")
    got = [swap(own, SPREAD, i) for i in range(chips - 1)] + [own]
    out = jnp.zeros((cores, chips) + own.shape, own.dtype)
    for i in (3, 0, 1, 2):
        there = lax.ppermute(got[i], "core", partners(2, 1))
        for c, row in ((core, got[i]), (1 - core, there)):
            out = lax.dynamic_update_slice(out, row[None, None], (c, chip ^ reach(SPREAD, c, i)) + (0,) * own.ndim)
    return out


def body(snapshots, validation, eigenvectors, eigenvalues):
    cores, chips = lax.axis_size("core"), lax.axis_size("chip")
    devices = cores * chips * lax.axis_size("plane")
    total = snapshots.shape[0] * devices * 1.0
    k, m = eigenvectors.shape
    piece = -(-layout(k, m)[-1] // (cores * chips * 8)) * 8
    e_rows, w_row = eigenvectors.T, eigenvalues[None, :]

    packed, modes, e_both, scales = head(snapshots, validation, e_rows, w_row, total, cores * chips * piece)
    own = reduce_scatter(packed.reshape(cores, chips, piece, LANES))
    own = all_reduce(own, "plane")
    packed = all_gather(own).reshape(-1, LANES)
    return tail(packed, modes, e_both, scales)


def solution(mesh):
    inner = axes_of(mesh)
    rows = ("plane", "chip", "core")
    in_specs = (P(rows, None), P(rows, None), P(), P())
    out_specs = (P(), P(None, rows), P(), P())
    step = jax.shard_map(body, mesh=inner, in_specs=in_specs, out_specs=out_specs, check_vma=False)
    if not all(direct(n) for n in inner.devices.shape):
        return step
    return step
```
